32 devices in a mesh: fsdp: 4 (over x, core), tm: 8 (over z, y).
Axes of the slice: x: 2, y: 2, z: 4, core: 2. Of those that a mesh axis runs over, the one named last changes fastest.
Arguments:
- tokens: bfloat16 [8, 8, 256, 1024], P('fsdp', 'tm'), may hold values from -6 to 6
- spatial_gain: float32 [1024], replicated, may hold values from 0.25 to 1.75
- spatial_qkv: bfloat16 [1024, 1536], P('fsdp'), may hold values from -16 to 16
- spatial_out: bfloat16 [512, 1024], P('fsdp'), may hold values from -0.25 to 0.25
- temporal_gain: float32 [1024], replicated, may hold values from 0.25 to 1.75
- temporal_qkv: bfloat16 [1024, 1536], P('fsdp'), may hold values from -16 to 16
- temporal_out: bfloat16 [512, 1024], P('fsdp'), may hold values from -0.25 to 0.25
Outputs:
- encoded: bfloat16 [8, 8, 256, 1024], P('fsdp', 'tm')
The draws below stay inside these ranges and needn't reach their ends.
All inputs are finite; a program needn't handle non-finite values.
Results may differ from the reference program's by a relative error of at most 0.0061.
Values may be sent and summed in bfloat16 or wider, within the bound.
A program may use at most 64 MiB of HBM per device.

```python
import jax
import jax.numpy as jnp
from jax import lax

D = 1024
HEAD = 64
HEADS = 8
P_SIZE = 256
INNER = 512
CLIPS = 8
FRAMES = 8


def drawn_weight(key):
    column_count = 3 * INNER
    sample = jax.random.normal(key, (D, column_count), jnp.float32) * D ** (-0.5)
    return jnp.clip(sample, -16.0, 16.0)


def draw_spatial_qkv(key, part):
    return drawn_weight(jax.random.fold_in(key, 11)).astype(jnp.bfloat16)


def draw_temporal_qkv(key, part):
    return drawn_weight(jax.random.fold_in(key, 23)).astype(jnp.bfloat16)


def draw_tokens(key, part):
    sample = jax.random.normal(jax.random.fold_in(key, 5), (CLIPS, FRAMES, P_SIZE, D), jnp.float32)
    return jnp.clip(sample, -6.0, 6.0).astype(jnp.bfloat16)


def shard_levels(rng, dims, shards, least, high):
    level, own = 1.0, jax.random.fold_in(rng, 6)
    for dim, parts in shards:
        heights = jnp.exp(jax.random.uniform(jax.random.fold_in(own, dim), (parts,), jnp.float32, least / len(shards), high / len(shards)))
        level = level * jnp.repeat(heights, dims[dim] // parts).reshape([-1 if axis == dim else 1 for axis in range(len(dims))])
    return level


def bell_draw(key, shape, scale, reach, cuts=(), dtype=jnp.bfloat16):
    level = shard_levels(key, shape, cuts, -0.22, 0.18) if cuts else 1.0
    result = jax.random.normal(key, shape, jnp.float32) * scale * level
    return jnp.minimum(jnp.maximum(result, -reach), reach).astype(dtype)


def setup_inputs(seed: int = 0) -> dict:
    arg_keys = jax.random.split(jax.random.key(seed), 8)
    return {
        "tokens": draw_tokens(jax.random.fold_in(arg_keys[7], 71), 0),
        "spatial_gain": jnp.clip(1.0 + 0.15 * jax.random.normal(arg_keys[1], (D,), jnp.float32), 0.25, 1.75),
        "spatial_qkv": draw_spatial_qkv(jax.random.fold_in(arg_keys[7], 71), 0),
        "spatial_out": bell_draw(arg_keys[3], (INNER, D), INNER ** -0.5, 0.25, ((0, 4),)),
        "temporal_gain": jnp.clip(1.0 + 0.15 * jax.random.normal(arg_keys[4], (D,), jnp.float32), 0.25, 1.75),
        "temporal_qkv": draw_temporal_qkv(jax.random.fold_in(arg_keys[7], 71), 0),
        "temporal_out": bell_draw(arg_keys[6], (INNER, D), INNER ** -0.5, 0.25, ((0, 4),)),
    }


EPSILON = 1e-06

def norm_rows(source, norm_gain):
    values = source.astype(jnp.float32)
    centre = values - lax.optimization_barrier(jnp.mean(values, axis=-1, keepdims=True))
    spread = lax.optimization_barrier(jnp.mean(centre * centre, axis=-1, keepdims=True))
    return (centre * lax.rsqrt(spread + EPSILON) * norm_gain).astype(jnp.bfloat16)

def attention_core(projected):
    inner_width = projected.shape[-1] // 3
    lead_shape = projected.shape[:-1]
    queries = projected[..., :inner_width].reshape(lead_shape + (HEADS, HEAD))
    key_rows = projected[..., inner_width:2 * inner_width].reshape(lead_shape + (HEADS, HEAD))
    value_rows = projected[..., 2 * inner_width:].astype(jnp.bfloat16).reshape(lead_shape + (HEADS, HEAD))
    scores = jnp.einsum('blmhe,bkmhe->bmhlk', queries, key_rows, precision=lax.Precision.HIGHEST) * HEAD ** (-0.5)
    row_max = lax.optimization_barrier(jnp.max(scores, axis=-1, keepdims=True))
    exponent = jnp.exp(scores - row_max)
    weights = (exponent / lax.optimization_barrier(jnp.sum(exponent, axis=-1, keepdims=True))).astype(jnp.bfloat16)
    context = jnp.einsum('bmhlk,bkmhe->blmhe', weights.astype(jnp.float32), value_rows.astype(jnp.float32), precision=lax.Precision.HIGHEST)
    return context.astype(jnp.bfloat16).reshape(lead_shape + (inner_width,))

def reference(tokens, spatial_gain, spatial_qkv, spatial_out, temporal_gain, temporal_qkv, temporal_out):

    def encode_clip(clip_tokens):
        frame_count, place_count, feature_width = clip_tokens.shape
        normed = norm_rows(clip_tokens, spatial_gain).reshape(-1, feature_width)
        projected = jnp.dot(normed, spatial_qkv, preferred_element_type=jnp.float32)
        context = attention_core(projected.reshape(frame_count, place_count, 1, 3 * INNER)).reshape(-1, INNER)
        middle = (clip_tokens.astype(jnp.float32).reshape(-1, feature_width) + jnp.dot(context, spatial_out, preferred_element_type=jnp.float32)).astype(jnp.bfloat16)
        normed_t = norm_rows(middle, temporal_gain)
        projected_t = jnp.dot(normed_t, temporal_qkv, preferred_element_type=jnp.float32)
        context_t = attention_core(projected_t.reshape(1, frame_count, place_count, 3 * INNER)).reshape(-1, INNER)
        encoded = middle.astype(jnp.float32) + jnp.dot(context_t, temporal_out, preferred_element_type=jnp.float32)
        return encoded.astype(jnp.bfloat16).reshape(frame_count, place_count, feature_width)
    return lax.map(encode_clip, tokens)
```

```python
import functools

import jax
import jax.numpy as jnp
from jax import lax
from jax.experimental import pallas as pl
from jax.experimental.pallas import tpu as pltpu
from jax.sharding import PartitionSpec as P

HEAD = 64
LANES = 128
EPSILON = 1e-06
MESH = pl.DeviceIdType.MESH
BF16 = jnp.bfloat16
F32 = jnp.float32


def pieces_of(depth):
    return max(2, depth // 32)


def crossed_of(w, depth):
    count = pieces_of(depth)
    return (count // 2, count // 2, count // 4, 0)[w]


def kernel(
    n_f, n_t, tok, sg, sqkv, sout, tg, tqkv, tout, out,
    xv, normed, proj, ctx, mid, arrived, normed_t, proj_t, ctx_t, ctx_back,
    wsq, wso, wtq, wto, outv,
    ack, ack_t, local_sem, w_local, w_send, w_recv, y_send, y_recv, m_send, m_recv, o_send, o_recv,
    p_send, p_recv, a_send, a_recv, c_send, c_recv, own_sem, out_sem,
):
    f = lax.axis_index("fsdp")
    t = lax.axis_index("tm")
    core = f % 2
    mate = f + 1 - 2 * core
    peers = n_f // 2 - 1
    half = n_t // 2
    side = t // half
    u = t % half
    partner = (t + half) % n_t
    keep = xv.shape[0] // 3
    rows, width = xv.shape[1:]
    inner = wso.shape[0]
    places = rows // half
    sends = []

    def start(cp):
        cp.start()
        sends.append(cp)

    barrier = pltpu.get_barrier_semaphore()
    for j in range(1, n_t):

        @pl.when(t + j < n_t)
        def _():
            pl.semaphore_signal(
                barrier, inc=1, device_id={"tm": (t + j) % n_t}, device_id_type=MESH
            )

    @pl.when(core == 0)
    def _():
        pl.semaphore_signal(barrier, inc=1, device_id={"fsdp": mate}, device_id_type=MESH)

    for k in range(peers):

        @pl.when(f + 2 * (k + 1) < n_f)
        def _():
            pl.semaphore_signal(
                barrier,
                inc=1,
                device_id={"fsdp": (f + 2 * (k + 1)) % n_f},
                device_id_type=MESH,
            )

    token_copies = []
    for c in range(keep):
        for slot, src in ((c, side * keep + c), (2 * keep + c, (1 - side) * keep + c)):
            cp = pltpu.make_async_copy(tok.at[src], xv.at[slot], local_sem.at[slot])
            cp.start()
            token_copies.append(cp)
    weights = ((sqkv, wsq), (sout, wso), (tqkv, wtq), (tout, wto))
    own_weights = []
    for w, (src, dst) in enumerate(weights):
        depth = src.shape[0]
        cp = pltpu.make_async_copy(src, dst.at[pl.ds(f * depth, depth)], w_local.at[w])
        cp.start()
        own_weights.append(cp)

    lower = t + core + f // 2

    @pl.when(lower > 0)
    def _():
        pl.semaphore_wait(barrier, lower)


    @pl.when(core == 1)
    def _():
        pl.semaphore_signal(ack.at[peers], inc=1, device_id={"fsdp": mate}, device_id_type=MESH)

    def source_of(who, k):
        return (who + n_f - 2 * (k + 1)) % n_f

    for k in range(peers):

        @pl.when(f >= 2 * (k + 1))
        def _():
            pl.semaphore_signal(
                ack.at[k], inc=1, device_id={"fsdp": source_of(f, k)}, device_id_type=MESH
            )

    for j in range(1, n_t):

        @pl.when(t >= j)
        def _():
            pl.semaphore_signal(
                ack_t.at[j], inc=1, device_id={"tm": (t + n_t - j) % n_t}, device_id_type=MESH
            )

    def entered(condition, j):
        @pl.when(condition)
        def _():
            pl.semaphore_wait(ack_t.at[j], 1)

    parity = t % 2
    beside = t + 1 - 2 * parity

    def rows_of(w, source, i, par):
        depth = weights[w][0].shape[0]
        count = pieces_of(depth)
        size = depth // count
        piece = i + par * (count - 1 - 2 * i)
        return pl.ds(pl.multiple_of(source * depth + piece * size, size), size)

    def direct(w, k, i, source):
        src, dst = weights[w]
        return pltpu.make_async_remote_copy(
            src_ref=src.at[rows_of(w, 0, i, parity)],
            dst_ref=dst.at[rows_of(w, source, i, parity)],
            send_sem=w_send.at[w, k, i],
            recv_sem=w_recv.at[w, k, i],
            device_id={"fsdp": (f + 2 * (k + 1)) % n_f},
            device_id_type=MESH,
        )

    def cross(w, k, i, source, par):
        dst = weights[w][1]
        where = rows_of(w, source, i, par)
        return pltpu.make_async_remote_copy(
            src_ref=dst.at[where],
            dst_ref=dst.at[where],
            send_sem=y_send.at[w, k, i],
            recv_sem=y_recv.at[w, k, i],
            device_id={"tm": beside},
            device_id_type=MESH,
        )

    def forward(w, k, i, source, par, slot):
        dst = weights[w][1]
        where = rows_of(w, source, i, par)
        return pltpu.make_async_remote_copy(
            src_ref=dst.at[where],
            dst_ref=dst.at[where],
            send_sem=m_send.at[w, k, slot],
            recv_sem=m_recv.at[w, k, slot],
            device_id={"fsdp": mate},
            device_id_type=MESH,
        )

    def mate_own(w, source):
        src, dst = weights[w]
        depth = src.shape[0]
        return pltpu.make_async_remote_copy(
            src_ref=src,
            dst_ref=dst.at[pl.ds(pl.multiple_of(source * depth, depth), depth)],
            send_sem=o_send.at[w],
            recv_sem=o_recv.at[w],
            device_id={"fsdp": mate},
            device_id_type=MESH,
        )

    def counts(w):
        depth = weights[w][0].shape[0]
        crossed = crossed_of(w, depth)
        return pieces_of(depth) - crossed, crossed

    def send_direct(w):
        for i in range(counts(w)[0]):
            for k in range(peers):
                start(direct(w, k, i, f))

    def relay(w, lo=0, hi=None):
        straight, crossed = counts(w)
        for i in range(lo, straight if hi is None else hi):
            for k in range(peers):
                source = source_of(f, k)
                direct(w, k, i, source).wait_recv()
                if i < crossed:
                    start(cross(w, k, i, source, parity))
                start(forward(w, k, i, source, parity, i))
        if hi is None:
            for i in range(crossed):
                for k in range(peers):
                    source = source_of(f, k)
                    cross(w, k, i, source, 1 - parity).wait_recv()
                    start(forward(w, k, i, source, 1 - parity, straight + i))

    def gathered(w):
        straight, crossed = counts(w)
        own_weights[w].wait()
        mate_own(w, mate).wait_recv()
        for k in range(peers):
            source = source_of(mate, k)
            for i in range(straight):
                forward(w, k, i, source, parity, i).wait_recv()
            for i in range(crossed):
                forward(w, k, i, source, 1 - parity, straight + i).wait_recv()

    def presend(c):
        return pltpu.make_async_remote_copy(
            src_ref=tok.at[(1 - side) * keep + c],
            dst_ref=xv.at[keep + c],
            send_sem=p_send.at[c],
            recv_sem=p_recv.at[c],
            device_id={"tm": partner},
            device_id_type=MESH,
        )

    def norm(values, gain):
        centre = values - jnp.mean(values, axis=-1, keepdims=True)
        spread = jnp.mean(centre * centre, axis=-1, keepdims=True)
        return (centre * lax.rsqrt(spread + EPSILON) * gain).astype(BF16)

    block = min(rows, 64)

    def norm_spatial(job):
        @pl.loop(0, rows // block)
        def _(i):
            where = pl.ds(pl.multiple_of(i * block, block), block)
            normed[job, where] = norm(xv[job, where].astype(F32), sg[...])

    def attend(read, size, same_place, store):
        lane = lax.broadcasted_iota(jnp.int32, (1, LANES), 1)
        first = lane < HEAD
        dims = (((1,), (1,)), ((), ()))

        @pl.loop(0, inner // LANES, unroll=4)
        def _(i):
            def load(offset):
                return read(pl.ds(pl.multiple_of(offset + i * LANES, LANES), LANES))

            q = load(0) * HEAD ** (-0.5)
            k = load(inner)
            v = load(2 * inner)
            qh = q.astype(BF16).astype(F32)
            ql = pltpu.roll(q - qh, HEAD, 1)
            kh = k.astype(BF16).astype(F32)
            kl = (k - kh).astype(BF16)
            kr = pltpu.roll(kh, HEAD, 1)
            parts = []
            for own in (first, jnp.logical_not(first)):
                high = jnp.where(own, qh, 0.0).astype(BF16)
                left = jnp.concatenate([jnp.where(own, qh, ql).astype(BF16), high], axis=1)
                right = jnp.concatenate([jnp.where(own, kh, kr).astype(BF16), kl], axis=1)
                s = lax.dot_general(left, right, dims, preferred_element_type=F32)
                if same_place is not None:
                    s = jnp.where(same_place, s, -1e30)
                e = jnp.exp(s - jnp.max(s, axis=-1, keepdims=True)).astype(BF16)
                ones = jnp.where(own, v, 1.0).astype(BF16)
                parts.append(jnp.dot(e, ones, preferred_element_type=F32))
            total = pltpu.roll(jnp.where(first, parts[1], parts[0]), HEAD, 1)
            result = jnp.where(first, parts[0], parts[1]) / total
            store(pl.ds(pl.multiple_of(i * LANES, LANES), LANES), result)

    def a2a(kind, c, j, to, frame):
        return pltpu.make_async_remote_copy(
            src_ref=mid.at[kind * keep + c, to % half],
            dst_ref=arrived.at[c, frame],
            send_sem=a_send.at[kind, c, j],
            recv_sem=a_recv.at[kind, c, j],
            device_id={"tm": to},
            device_id_type=MESH,
        )

    def own_mid(kind, c):
        frame = t if kind == 0 else partner
        return pltpu.make_async_copy(
            mid.at[kind * keep + c, u], arrived.at[c, frame], own_sem.at[kind, c]
        )

    def within(j):
        return side * half + (u + j) % half

    def send_mid(kind, c):
        for j in range(1, half):
            a2a(kind, c, j, within(j), t if kind == 0 else partner).start()
        own_mid(kind, c).start()

    def spatial(job):
        @pl.loop(0, 3)
        def _(i):
            cols = pl.ds(pl.multiple_of(i * inner, LANES), inner)
            proj[:, cols] = jnp.dot(normed[job], wsq[:, cols], preferred_element_type=F32)

        def store(cols, result):
            ctx[:, cols] = result.astype(BF16)

        attend(lambda cols: proj[:, cols], rows, None, store)

    def spatial_out(job):
        @pl.loop(0, width // inner)
        def _(i):
            cols = pl.ds(pl.multiple_of(i * inner, LANES), inner)
            part = xv[job, :, cols].astype(F32) + jnp.dot(
                ctx[...], wso[:, cols], preferred_element_type=F32
            )
            mid[job, :, :, cols] = part.reshape(half, places, inner).astype(BF16)

    @pl.when(core == 1)
    def _():
        for w in range(4):
            mate_own(w, f).start()

    for k in range(peers):

        @pl.when(f + 2 * (k + 1) < n_f)
        def _():
            pl.semaphore_wait(ack.at[k], 1)

    for w in range(4):
        send_direct(w)
    for cp in token_copies:
        cp.wait()
    for c in range(keep):
        norm_spatial(c)

    @pl.when(core == 0)
    def _():
        pl.semaphore_wait(ack.at[peers], 1)
        for w in range(4):
            mate_own(w, f).start()

    entered(t < half, half)

    @pl.when(core == 0)
    def _():
        for c in range(keep):
            presend(c).start()

    entered(parity == 0, 1)
    for c in range(keep):
        norm_spatial(2 * keep + c)

    relay(0)
    gathered(0)

    @pl.when(core == 1)
    def _():
        for c in range(keep):
            presend(c).start()

    for j in range(1, half):
        entered((u + j < half) & ((parity == 1) | (j > 1)), j)
    for c in range(keep):
        spatial(c)
        if c == 0:
            relay(1)
            gathered(1)
        spatial_out(c)
        send_mid(0, c)

    straight = counts(2)[0]
    relay(2, 0, straight // 3)

    def foreign(c):
        presend(c).wait_recv()
        norm_spatial(keep + c)

    for step in range(2):
        for c in range(keep):
            kind = 1 + core if step == 0 else 2 - core
            job = kind * keep + c

            @pl.when(kind == 1)
            def _():
                foreign(c)

            spatial(job)
            spatial_out(job)

            @pl.when(kind == 1)
            def _():
                send_mid(1, c)

        if step == 0:
            relay(2, straight // 3, 2 * straight // 3)
    relay(2, 2 * straight // 3)

    steps = max(1, places // 32)
    chunk = places // steps
    group = min(chunk, max(8, LANES // n_t))
    size = n_t * group
    r = lax.rem(lax.broadcasted_iota(jnp.int32, (size, 1), 0), group)
    l = lax.rem(lax.broadcasted_iota(jnp.int32, (1, size), 1), group)
    same_place = r == l

    def back(c, s, j, to, clip, slot):
        lo = s * chunk
        return pltpu.make_async_remote_copy(
            src_ref=ctx_t.at[c, to, pl.ds(lo, chunk)],
            dst_ref=ctx_back.at[clip, slot, pl.ds(lo, chunk)],
            send_sem=c_send.at[c, s, j],
            recv_sem=c_recv.at[c, s, j],
            device_id={"tm": to},
            device_id_type=MESH,
        )

    def own_back(c, s):
        lo = s * chunk
        return pltpu.make_async_copy(
            ctx_t.at[c, t, pl.ds(lo, chunk)],
            ctx_back.at[side * keep + c, u, pl.ds(lo, chunk)],
            own_sem.at[2 + s, c],
        )

    for j in range(1, n_t):
        if j != half:
            entered((t + j < n_t) & (u + j >= half), j)
    far_first = sorted(range(1, n_t), key=lambda j: abs(j - half))
    for c in range(keep):
        for kind in range(2):
            own_mid(kind, c).wait()
            for j in range(1, half):
                source = within(half - j)
                frame = source if kind == 0 else (source + half) % n_t
                a2a(kind, c, j, within(j), frame).wait_recv()
        for s in range(steps):
            lo = s * chunk
            span = max(1, block // chunk)

            @pl.loop(0, n_t // span)
            def _(i):
                frames = pl.ds(i * span, span)
                values = arrived[c, frames, lo : lo + chunk].astype(F32)
                values = norm(values.reshape(span * chunk, width), tg[...])
                where = pl.ds(pl.multiple_of(i * span * chunk, span * chunk), span * chunk)
                normed_t[where] = values

            if c == 0 and s == 0:
                gathered(2)

            @pl.loop(0, 3)
            def _(i):
                cols = pl.ds(pl.multiple_of(i * inner, LANES), inner)
                part = jnp.dot(normed_t[...], wtq[:, cols], preferred_element_type=F32)
                proj_t[:, :, cols] = part.reshape(n_t, chunk, inner)

            for g in range(chunk // group):
                at = g * group

                def store(cols, result):
                    ctx_t[c, :, lo + at : lo + at + group, cols] = result.reshape(
                        n_t, group, LANES
                    ).astype(BF16)

                attend(
                    lambda cols: proj_t[:, at : at + group, cols].reshape(size, LANES),
                    size, same_place, store,
                )
            for j in far_first:
                start(back(c, s, j, (t + j) % n_t, side * keep + c, u))
            own_back(c, s).start()
    relay(3)
    gathered(3)

    finals = []
    for far in (False, True):
        clip_side = 1 - side if far else side
        for c in range(keep):
            clip = clip_side * keep + c
            job = (2 if far else 0) * keep + c
            for s in range(steps):
                lo = s * chunk
                if not far:
                    own_back(c, s).wait()
                for j in range(1, n_t):
                    source = (t + n_t - j) % n_t

                    @pl.when((source // half == side) != far)
                    def _():
                        back(c, s, j, (t + j) % n_t, clip, source % half).wait_recv()

                part_rows = half * chunk
                now = ctx_back[clip, :, lo : lo + chunk].reshape(part_rows, inner)

                @pl.loop(0, width // inner)
                def _(i):
                    cols = pl.ds(pl.multiple_of(i * inner, LANES), inner)
                    base = mid[job, :, lo : lo + chunk, cols].astype(F32)
                    part = base.reshape(part_rows, inner) + jnp.dot(
                        now, wto[:, cols], preferred_element_type=F32
                    )
                    outv[far * keep + c, :, lo : lo + chunk, cols] = part.reshape(
                        half, chunk, inner
                    ).astype(BF16)

            cp = pltpu.make_async_copy(outv.at[far * keep + c], out.at[clip], out_sem.at[far * keep + c])
            cp.start()
            finals.append(cp)

    for c in range(keep):
        presend(c).wait_send()
        for kind in range(2):
            for j in range(1, half):
                a2a(kind, c, j, within(j), t).wait_send()
    for w in range(4):
        mate_own(w, f).wait_send()
    for cp in sends:
        cp.wait_send()
    for cp in finals:
        cp.wait()


def shards(
    n_f, n_t, tokens, spatial_gain, spatial_qkv, spatial_out, temporal_gain, temporal_qkv,
    temporal_out,
):
    clip_count, frames, rows, width = tokens.shape
    assert frames == 1 and clip_count % 2 == 0 and n_t % 4 == 0
    inner = spatial_out.shape[0] * n_f
    columns = spatial_qkv.shape[1]
    keep = clip_count // 2
    half = n_t // 2
    places = rows // half
    steps = max(1, places // 32)
    chunk = places // steps
    peers = max(1, n_f // 2 - 1)
    most = pieces_of(max(spatial_qkv.shape[0], spatial_out.shape[0]))
    anywhere = pl.BlockSpec(memory_space=pl.ANY)
    vmem = pl.BlockSpec(memory_space=pltpu.VMEM)
    dma = pltpu.SemaphoreType.DMA
    result = pl.pallas_call(
        functools.partial(kernel, n_f, n_t),
        out_shape=jax.ShapeDtypeStruct((clip_count, half, places, width), BF16),
        in_specs=[anywhere, vmem, anywhere, anywhere, vmem, anywhere, anywhere],
        out_specs=anywhere,
        scratch_shapes=[
            pltpu.VMEM((3 * keep, rows, width), BF16),
            pltpu.VMEM((3 * keep, rows, width), BF16),
            pltpu.VMEM((rows, columns), F32),
            pltpu.VMEM((rows, inner), BF16),
            pltpu.VMEM((3 * keep, half, places, width), BF16),
            pltpu.VMEM((keep, n_t, places, width), BF16),
            pltpu.VMEM((n_t * chunk, width), BF16),
            pltpu.VMEM((n_t, chunk, columns), F32),
            pltpu.VMEM((keep, n_t, places, inner), BF16),
            pltpu.VMEM((clip_count, half, places, inner), BF16),
            pltpu.VMEM((width, columns), BF16),
            pltpu.VMEM((inner, width), BF16),
            pltpu.VMEM((width, columns), BF16),
            pltpu.VMEM((inner, width), BF16),
            pltpu.VMEM((clip_count, half, places, width), BF16),
            pltpu.SemaphoreType.REGULAR((peers + 1,)),
            pltpu.SemaphoreType.REGULAR((n_t,)),
            dma((3 * keep,)),
            dma((4,)),
            dma((4, peers, most)),
            dma((4, peers, most)),
            dma((4, peers, most)),
            dma((4, peers, most)),
            dma((4, peers, most)),
            dma((4, peers, most)),
            dma((4,)),
            dma((4,)),
            dma((keep,)),
            dma((keep,)),
            dma((2, keep, half)),
            dma((2, keep, half)),
            dma((keep, steps, n_t)),
            dma((keep, steps, n_t)),
            dma((2 + steps, keep)),
            dma((clip_count,)),
        ],
        compiler_params=pltpu.CompilerParams(
            collective_id=0, has_side_effects=True, vmem_limit_bytes=67000000
        ),
    )(
        tokens.reshape(clip_count, rows, width),
        spatial_gain.reshape(1, width),
        spatial_qkv,
        spatial_out,
        temporal_gain.reshape(1, width),
        temporal_qkv,
        temporal_out,
    )
    return result.reshape(clip_count, frames, rows, width)


def solution(mesh):
    placed = (
        P("fsdp", "tm", None, None),
        P(),
        P("fsdp", None),
        P("fsdp", None),
        P(),
        P("fsdp", None),
        P("fsdp", None),
    )
    body = functools.partial(shards, mesh.shape["fsdp"], mesh.shape["tm"])
    return jax.shard_map(
        body, mesh=mesh, in_specs=placed, out_specs=P("fsdp", "tm", None, None), check_vma=False
    )
```

```python
import functools

import jax
import jax.numpy as jnp
from jax import lax
from jax.experimental import pallas as pl
from jax.experimental.pallas import tpu as pltpu
from jax.sharding import PartitionSpec as P

HEAD = 64
LANES = 128
EPSILON = 1e-06
MESH = pl.DeviceIdType.MESH
BF16 = jnp.bfloat16
F32 = jnp.float32


def pieces_of(depth):
    return max(2, depth // 64)


def crossed_of(w, depth):
    count = pieces_of(depth)
    return (count // 2, 0, 0, 0)[w]


def kernel(
    n_f, n_t, tok, sg, sqkv, sout, tg, tqkv, tout, out,
    xv, normed, proj, ctx, mid, arrived, normed_t, proj_t, ctx_t, ctx_back,
    wsq, wso, wtq, wto, outv,
    ack, ack_t, local_sem, w_local, w_send, w_recv, y_send, y_recv, m_send, m_recv, o_send, o_recv,
    p_send, p_recv, a_send, a_recv, c_send, c_recv, own_sem, out_sem,
):
    f = lax.axis_index("fsdp")
    t = lax.axis_index("tm")
    core = f % 2
    mate = f + 1 - 2 * core
    peers = n_f // 2 - 1
    half = n_t // 2
    side = t // half
    u = t % half
    partner = (t + half) % n_t
    first_clip = side * (1 - core)
    rows, width = xv.shape[1:]
    inner = wso.shape[0]
    places = rows // n_t
    sends = []

    def start(cp):
        cp.start()
        sends.append(cp)

    barrier = pltpu.get_barrier_semaphore()
    for j in range(1, n_t):

        @pl.when(t + j < n_t)
        def _():
            pl.semaphore_signal(
                barrier, inc=1, device_id={"tm": (t + j) % n_t}, device_id_type=MESH
            )

    @pl.when(core == 0)
    def _():
        pl.semaphore_signal(barrier, inc=1, device_id={"fsdp": mate}, device_id_type=MESH)

    for k in range(peers):

        @pl.when(f + 2 * (k + 1) < n_f)
        def _():
            pl.semaphore_signal(
                barrier,
                inc=1,
                device_id={"fsdp": (f + 2 * (k + 1)) % n_f},
                device_id_type=MESH,
            )

    token_copies = []
    for slot, src in ((0, first_clip), (2, 1 - first_clip)):
        cp = pltpu.make_async_copy(tok.at[src], xv.at[slot], local_sem.at[slot])
        cp.start()
        token_copies.append(cp)
    weights = ((sqkv, wsq), (sout, wso), (tqkv, wtq), (tout, wto))
    own_weights = []
    for w, (src, dst) in enumerate(weights):
        depth = src.shape[0]
        cp = pltpu.make_async_copy(src, dst.at[pl.ds(f * depth, depth)], w_local.at[w])
        cp.start()
        own_weights.append(cp)

    lower = t + core + f // 2

    @pl.when(lower > 0)
    def _():
        pl.semaphore_wait(barrier, lower)


    @pl.when(core == 1)
    def _():
        pl.semaphore_signal(ack.at[peers], inc=1, device_id={"fsdp": mate}, device_id_type=MESH)

    def source_of(who, k):
        return (who + n_f - 2 * (k + 1)) % n_f

    for k in range(peers):

        @pl.when(f >= 2 * (k + 1))
        def _():
            pl.semaphore_signal(
                ack.at[k], inc=1, device_id={"fsdp": source_of(f, k)}, device_id_type=MESH
            )

    for j in range(1, n_t):

        @pl.when(t >= j)
        def _():
            pl.semaphore_signal(
                ack_t.at[j], inc=1, device_id={"tm": (t + n_t - j) % n_t}, device_id_type=MESH
            )

    def entered(condition, j):
        @pl.when(condition)
        def _():
            pl.semaphore_wait(ack_t.at[j], 1)

    parity = t % 2
    beside = t + 1 - 2 * parity

    def rows_of(w, source, i, par):
        depth = weights[w][0].shape[0]
        count = pieces_of(depth)
        size = depth // count
        piece = i + par * (count - 1 - 2 * i)
        return pl.ds(pl.multiple_of(source * depth + piece * size, size), size)

    def direct(w, k, i, source):
        src, dst = weights[w]
        return pltpu.make_async_remote_copy(
            src_ref=src.at[rows_of(w, 0, i, parity)],
            dst_ref=dst.at[rows_of(w, source, i, parity)],
            send_sem=w_send.at[w, k, i],
            recv_sem=w_recv.at[w, k, i],
            device_id={"fsdp": (f + 2 * (k + 1)) % n_f},
            device_id_type=MESH,
        )

    def cross(w, k, i, source, par):
        dst = weights[w][1]
        where = rows_of(w, source, i, par)
        return pltpu.make_async_remote_copy(
            src_ref=dst.at[where],
            dst_ref=dst.at[where],
            send_sem=y_send.at[w, k, i],
            recv_sem=y_recv.at[w, k, i],
            device_id={"tm": beside},
            device_id_type=MESH,
        )

    def forward(w, k, i, source, par, slot):
        dst = weights[w][1]
        where = rows_of(w, source, i, par)
        return pltpu.make_async_remote_copy(
            src_ref=dst.at[where],
            dst_ref=dst.at[where],
            send_sem=m_send.at[w, k, slot],
            recv_sem=m_recv.at[w, k, slot],
            device_id={"fsdp": mate},
            device_id_type=MESH,
        )

    def mate_own(w, source):
        src, dst = weights[w]
        depth = src.shape[0]
        return pltpu.make_async_remote_copy(
            src_ref=src,
            dst_ref=dst.at[pl.ds(pl.multiple_of(source * depth, depth), depth)],
            send_sem=o_send.at[w],
            recv_sem=o_recv.at[w],
            device_id={"fsdp": mate},
            device_id_type=MESH,
        )

    def counts(w):
        depth = weights[w][0].shape[0]
        crossed = crossed_of(w, depth)
        return pieces_of(depth) - crossed, crossed

    def send_direct(w):
        for i in range(counts(w)[0]):
            for k in range(peers):
                start(direct(w, k, i, f))

    def relay(w, lo=0, hi=None):
        straight, crossed = counts(w)
        for i in range(lo, straight if hi is None else hi):
            for k in range(peers):
                source = source_of(f, k)
                direct(w, k, i, source).wait_recv()
                if i < crossed:
                    start(cross(w, k, i, source, parity))
                start(forward(w, k, i, source, parity, i))
        if hi is None:
            for i in range(crossed):
                for k in range(peers):
                    source = source_of(f, k)
                    cross(w, k, i, source, 1 - parity).wait_recv()
                    start(forward(w, k, i, source, 1 - parity, straight + i))

    def gathered(w):
        straight, crossed = counts(w)
        own_weights[w].wait()
        mate_own(w, mate).wait_recv()
        for k in range(peers):
            source = source_of(mate, k)
            for i in range(straight):
                forward(w, k, i, source, parity, i).wait_recv()
            for i in range(crossed):
                forward(w, k, i, source, 1 - parity, straight + i).wait_recv()

    def presend():
        return pltpu.make_async_remote_copy(
            src_ref=tok.at[1 - side],
            dst_ref=xv.at[1],
            send_sem=p_send,
            recv_sem=p_recv,
            device_id={"tm": partner},
            device_id_type=MESH,
        )

    def norm(values, gain):
        centre = values - jnp.mean(values, axis=-1, keepdims=True)
        spread = jnp.mean(centre * centre, axis=-1, keepdims=True)
        return (centre * lax.rsqrt(spread + EPSILON) * gain).astype(BF16)

    block = min(rows, 64)

    def norm_spatial(job):
        @pl.loop(0, rows // block)
        def _(i):
            where = pl.ds(pl.multiple_of(i * block, block), block)
            normed[job, where] = norm(xv[job, where].astype(F32), sg[...])

    def attend(read, size, same_place, store):
        lane = lax.broadcasted_iota(jnp.int32, (1, LANES), 1)
        first = lane < HEAD
        dims = (((1,), (1,)), ((), ()))

        @pl.loop(0, inner // LANES, unroll=4)
        def _(i):
            def load(offset):
                return read(pl.ds(pl.multiple_of(offset + i * LANES, LANES), LANES))

            q = load(0) * HEAD ** (-0.5)
            k = load(inner)
            v = load(2 * inner)
            qh = q.astype(BF16).astype(F32)
            ql = pltpu.roll(q - qh, HEAD, 1)
            kh = k.astype(BF16).astype(F32)
            kl = (k - kh).astype(BF16)
            kr = pltpu.roll(kh, HEAD, 1)
            parts = []
            for own in (first, jnp.logical_not(first)):
                high = jnp.where(own, qh, 0.0).astype(BF16)
                left = jnp.concatenate([jnp.where(own, qh, ql).astype(BF16), high], axis=1)
                right = jnp.concatenate([jnp.where(own, kh, kr).astype(BF16), kl], axis=1)
                s = lax.dot_general(left, right, dims, preferred_element_type=F32)
                if same_place is not None:
                    s = jnp.where(same_place, s, -1e30)
                e = jnp.exp(s - jnp.max(s, axis=-1, keepdims=True)).astype(BF16)
                ones = jnp.where(own, v, 1.0).astype(BF16)
                parts.append(jnp.dot(e, ones, preferred_element_type=F32))
            total = pltpu.roll(jnp.where(first, parts[1], parts[0]), HEAD, 1)
            result = jnp.where(first, parts[0], parts[1]) / total
            store(pl.ds(pl.multiple_of(i * LANES, LANES), LANES), result)

    def a2a(kind, s, j, job, to, take, frame):
        return pltpu.make_async_remote_copy(
            src_ref=mid.at[job, take],
            dst_ref=arrived.at[s, frame],
            send_sem=a_send.at[kind, s, j],
            recv_sem=a_recv.at[kind, s, j],
            device_id={"tm": to},
            device_id_type=MESH,
        )

    def own_mid(kind, s, job, take, frame):
        return pltpu.make_async_copy(
            mid.at[job, take], arrived.at[s, frame], own_sem.at[kind, s]
        )

    far_first = sorted(range(1, n_t), key=lambda j: abs(j - half))

    def near(kind, act):
        frame = (t, partner)[kind]
        for s in range(2):
            for j in range(1, half):
                there = (u + j) % half
                act(a2a(kind, s, j, kind, side * half + there, 2 * there + s, frame))
            if act is begin:
                own_mid(kind, s, kind, 2 * u + s, frame).start()

    def wide(s, act):
        job = 2 * s
        for j in far_first:
            to = (t + j) % n_t
            act(a2a(0, s, j, job, to, to, t))
        if act is begin:
            own_mid(0, s, job, t, t).start()

    def begin(cp):
        cp.start()

    def drain(cp):
        cp.wait_send()

    def arrive(s):
        @pl.when(core == 0)
        def _():
            for kind in range(2):
                own_mid(kind, s, kind, 2 * u + s, (t, partner)[kind]).wait()
                for j in range(1, half):
                    source = side * half + (u + half - j) % half
                    frame = (source, (source + half) % n_t)[kind]
                    a2a(kind, s, j, kind, source, 0, frame).wait_recv()

        @pl.when(core == 1)
        def _():
            own_mid(0, s, 2 * s, t, t).wait()
            for j in range(1, n_t):
                source = (t + n_t - j) % n_t
                a2a(0, s, j, 2 * s, source, 0, source).wait_recv()

    def spatial(job):
        @pl.loop(0, 3)
        def _(i):
            cols = pl.ds(pl.multiple_of(i * inner, LANES), inner)
            proj[:, cols] = jnp.dot(normed[job], wsq[:, cols], preferred_element_type=F32)

        def store(cols, result):
            ctx[:, cols] = result.astype(BF16)

        attend(lambda cols: proj[:, cols], rows, None, store)

    def spatial_out(job):
        @pl.loop(0, width // inner)
        def _(i):
            cols = pl.ds(pl.multiple_of(i * inner, LANES), inner)
            part = xv[job, :, cols].astype(F32) + jnp.dot(
                ctx[...], wso[:, cols], preferred_element_type=F32
            )
            mid[job, :, :, cols] = part.reshape(n_t, places, inner).astype(BF16)

    @pl.when(core == 1)
    def _():
        for w in range(4):
            mate_own(w, f).start()

    for k in range(peers):

        @pl.when(f + 2 * (k + 1) < n_f)
        def _():
            pl.semaphore_wait(ack.at[k], 1)

    for w in range(4):
        send_direct(w)
    entered(t < half, half)

    @pl.when(core == 0)
    def _():
        presend().start()

    token_copies[0].wait()
    norm_spatial(0)

    @pl.when(core == 0)
    def _():
        pl.semaphore_wait(ack.at[peers], 1)
        for w in range(4):
            mate_own(w, f).start()

    entered(parity == 0, 1)
    token_copies[1].wait()
    norm_spatial(2)

    relay(0)
    gathered(0)
    for j in range(1, n_t):
        if j != half:
            entered((t + j < n_t) & ((parity == 1) | (j > 1)), j)

    spatial(0)
    relay(1)
    gathered(1)
    spatial_out(0)

    @pl.when(core == 0)
    def _():
        near(0, begin)

    @pl.when(core == 1)
    def _():
        wide(0, begin)

    straight = counts(2)[0]
    relay(2, 0, straight // 3)

    @pl.when(core == 0)
    def _():
        presend().wait_recv()
        norm_spatial(1)

    spatial(1 + core)
    spatial_out(1 + core)

    @pl.when(core == 0)
    def _():
        near(1, begin)

    @pl.when(core == 1)
    def _():
        wide(1, begin)

    relay(2, straight // 3, 2 * straight // 3)

    @pl.when(core == 0)
    def _():
        spatial(2)
        spatial_out(2)

    relay(2, 2 * straight // 3)

    group = min(places, max(8, LANES // n_t))
    size = n_t * group
    r = lax.rem(lax.broadcasted_iota(jnp.int32, (size, 1), 0), group)
    l = lax.rem(lax.broadcasted_iota(jnp.int32, (1, size), 1), group)
    same_place = r == l

    def back(s, j, to, clip, slot):
        return pltpu.make_async_remote_copy(
            src_ref=ctx_t.at[s, to],
            dst_ref=ctx_back.at[clip, slot],
            send_sem=c_send.at[s, j],
            recv_sem=c_recv.at[s, j],
            device_id={"tm": to},
            device_id_type=MESH,
        )

    def place_of(s):
        return side * (1 - core) + s * core, (2 * u + s) * (1 - core) + t * core

    def own_back(s):
        clip, slot = place_of(s)
        return pltpu.make_async_copy(ctx_t.at[s, t], ctx_back.at[clip, slot], own_sem.at[2, s])

    span = max(1, block // places)
    for s in range(2):
        arrive(s)

        @pl.loop(0, n_t // span)
        def _(i):
            frames = pl.ds(i * span, span)
            values = arrived[s, frames].astype(F32).reshape(span * places, width)
            where = pl.ds(pl.multiple_of(i * span * places, span * places), span * places)
            normed_t[where] = norm(values, tg[...])

        if s == 0:
            gathered(2)

        @pl.loop(0, 3)
        def _(i):
            cols = pl.ds(pl.multiple_of(i * inner, LANES), inner)
            part = jnp.dot(normed_t[...], wtq[:, cols], preferred_element_type=F32)
            proj_t[:, :, cols] = part.reshape(n_t, places, inner)

        for g in range(places // group):
            at = g * group

            def store(cols, result):
                ctx_t[s, :, at : at + group, cols] = result.reshape(n_t, group, LANES).astype(
                    BF16
                )

            attend(
                lambda cols: proj_t[:, at : at + group, cols].reshape(size, LANES),
                size, same_place, store,
            )
        clip, slot = place_of(s)
        for j in far_first:
            back(s, j, (t + j) % n_t, clip, slot).start()
        own_back(s).start()
        if s == 0:
            relay(3)
    gathered(3)
    for cp in sends:
        cp.wait_send()
    for w in range(4):
        mate_own(w, f).wait_send()

    @pl.when(core == 0)
    def _():
        presend().wait_send()
        near(0, drain)
        near(1, drain)

    @pl.when(core == 1)
    def _():
        wide(0, drain)
        wide(1, drain)

    finals = []
    for e in range(2):
        clip = first_clip if e == 0 else 1 - first_clip

        @pl.when(core == 0)
        def _():
            for s in range(2):
                if e == 0:
                    own_back(s).wait()
                for j in range(1, n_t):
                    source = (t + n_t - j) % n_t

                    @pl.when((source // half == side) == (e == 0))
                    def _():
                        back(s, j, source, source // half, 2 * (source % half) + s).wait_recv()

        @pl.when(core == 1)
        def _():
            own_back(e).wait()
            for j in range(1, n_t):
                source = (t + n_t - j) % n_t
                back(e, j, source, e, source).wait_recv()

        now = ctx_back[clip]
        if places % 16:
            now = now.astype(F32)
        ctx[...] = now.reshape(rows, inner).astype(BF16)

        @pl.loop(0, width // inner)
        def _(i):
            cols = pl.ds(pl.multiple_of(i * inner, LANES), inner)
            base = mid[2 * e, :, :, cols].astype(F32).reshape(rows, inner)
            part = base + jnp.dot(ctx[...], wto[:, cols], preferred_element_type=F32)
            outv[e, :, :, cols] = part.reshape(n_t, places, inner).astype(BF16)

        cp = pltpu.make_async_copy(outv.at[e], out.at[clip], out_sem.at[e])
        cp.start()
        finals.append(cp)
    for s in range(2):
        for j in range(1, n_t):
            back(s, j, (t + j) % n_t, 0, 0).wait_send()
    for cp in finals:
        cp.wait()


def shards(
    n_f, n_t, tokens, spatial_gain, spatial_qkv, spatial_out, temporal_gain, temporal_qkv,
    temporal_out,
):
    clip_count, frames, rows, width = tokens.shape
    assert frames == 1 and clip_count == 2 and n_t % 4 == 0
    inner = spatial_out.shape[0] * n_f
    columns = spatial_qkv.shape[1]
    half = n_t // 2
    places = rows // n_t
    peers = max(1, n_f // 2 - 1)
    most = pieces_of(max(spatial_qkv.shape[0], spatial_out.shape[0]))
    anywhere = pl.BlockSpec(memory_space=pl.ANY)
    vmem = pl.BlockSpec(memory_space=pltpu.VMEM)
    dma = pltpu.SemaphoreType.DMA
    result = pl.pallas_call(
        functools.partial(kernel, n_f, n_t),
        out_shape=jax.ShapeDtypeStruct((clip_count, n_t, places, width), BF16),
        in_specs=[anywhere, vmem, anywhere, anywhere, vmem, anywhere, anywhere],
        out_specs=anywhere,
        scratch_shapes=[
            pltpu.VMEM((3, rows, width), BF16),
            pltpu.VMEM((3, rows, width), BF16),
            pltpu.VMEM((rows, columns), F32),
            pltpu.VMEM((rows, inner), BF16),
            pltpu.VMEM((3, n_t, places, width), BF16),
            pltpu.VMEM((2, n_t, places, width), BF16),
            pltpu.VMEM((rows, width), BF16),
            pltpu.VMEM((n_t, places, columns), F32),
            pltpu.VMEM((2, n_t, places, inner), BF16),
            pltpu.VMEM((2, n_t, places, inner), BF16),
            pltpu.VMEM((width, columns), BF16),
            pltpu.VMEM((inner, width), BF16),
            pltpu.VMEM((width, columns), BF16),
            pltpu.VMEM((inner, width), BF16),
            pltpu.VMEM((2, n_t, places, width), BF16),
            pltpu.SemaphoreType.REGULAR((peers + 1,)),
            pltpu.SemaphoreType.REGULAR((n_t,)),
            dma((3,)),
            dma((4,)),
            dma((4, peers, most)),
            dma((4, peers, most)),
            dma((4, peers, most)),
            dma((4, peers, most)),
            dma((4, peers, most)),
            dma((4, peers, most)),
            dma((4,)),
            dma((4,)),
            dma,
            dma,
            dma((2, 2, n_t)),
            dma((2, 2, n_t)),
            dma((2, n_t)),
            dma((2, n_t)),
            dma((3, 2)),
            dma((2,)),
        ],
        compiler_params=pltpu.CompilerParams(
            collective_id=0, has_side_effects=True, vmem_limit_bytes=67000000
        ),
    )(
        tokens.reshape(clip_count, rows, width),
        spatial_gain.reshape(1, width),
        spatial_qkv,
        spatial_out,
        temporal_gain.reshape(1, width),
        temporal_qkv,
        temporal_out,
    )
    return result.reshape(clip_count, frames, rows, width)


def solution(mesh):
    placed = (
        P("fsdp", "tm", None, None),
        P(),
        P("fsdp", None),
        P("fsdp", None),
        P(),
        P("fsdp", None),
        P("fsdp", None),
    )
    body = functools.partial(shards, mesh.shape["fsdp"], mesh.shape["tm"])
    return jax.shard_map(
        body, mesh=mesh, in_specs=placed, out_specs=P("fsdp", "tm", None, None), check_vma=False
    )
```

```python
import functools

import jax
import jax.numpy as jnp
from jax import lax
from jax.experimental import pallas as pl
from jax.experimental.pallas import tpu as pltpu
from jax.sharding import PartitionSpec as P

HEAD = 64
LANES = 128
EPSILON = 1e-06
MESH = pl.DeviceIdType.MESH
BF16 = jnp.bfloat16
F32 = jnp.float32


def pieces_of(depth):
    return max(2, depth // 64)


def crossed_of(w, depth):
    count = pieces_of(depth)
    return (count // 2, 0, 0, 0)[w]


def kernel(
    n_f, n_t, tok, sg, sqkv, sout, tg, tqkv, tout, out,
    xv, normed, proj, ctx, mid, arrived, normed_t, proj_t, ctx_t, ctx_back,
    wsq, wso, wtq, wto, outv,
    ack, ack_t, local_sem, w_local, w_send, w_recv, y_send, y_recv, m_send, m_recv, o_send, o_recv,
    p_send, p_recv, a_send, a_recv, c_send, c_recv, own_sem, out_sem,
):
    f = lax.axis_index("fsdp")
    t = lax.axis_index("tm")
    core = f % 2
    mate = f + 1 - 2 * core
    peers = n_f // 2 - 1
    half = n_t // 2
    side = t // half
    u = t % half
    partner = (t + half) % n_t
    first_clip = side * (1 - core)
    rows, width = xv.shape[1:]
    inner = wso.shape[0]
    places = rows // n_t
    sends = []

    def start(cp):
        cp.start()
        sends.append(cp)

    barrier = pltpu.get_barrier_semaphore()
    for j in range(1, n_t):

        @pl.when(t + j < n_t)
        def _():
            pl.semaphore_signal(
                barrier, inc=1, device_id={"tm": (t + j) % n_t}, device_id_type=MESH
            )

    @pl.when(core == 0)
    def _():
        pl.semaphore_signal(barrier, inc=1, device_id={"fsdp": mate}, device_id_type=MESH)

    for k in range(peers):

        @pl.when(f + 2 * (k + 1) < n_f)
        def _():
            pl.semaphore_signal(
                barrier,
                inc=1,
                device_id={"fsdp": (f + 2 * (k + 1)) % n_f},
                device_id_type=MESH,
            )

    token_copies = []
    for slot, src in ((0, first_clip), (2, 1 - first_clip)):
        cp = pltpu.make_async_copy(tok.at[src], xv.at[slot], local_sem.at[slot])
        cp.start()
        token_copies.append(cp)
    weights = ((sqkv, wsq), (sout, wso), (tqkv, wtq), (tout, wto))
    own_weights = []
    for w, (src, dst) in enumerate(weights):
        depth = src.shape[0]
        cp = pltpu.make_async_copy(src, dst.at[pl.ds(f * depth, depth)], w_local.at[w])
        cp.start()
        own_weights.append(cp)

    lower = t + core + f // 2

    @pl.when(lower > 0)
    def _():
        pl.semaphore_wait(barrier, lower)


    @pl.when(core == 1)
    def _():
        pl.semaphore_signal(ack.at[peers], inc=1, device_id={"fsdp": mate}, device_id_type=MESH)

    def source_of(who, k):
        return (who + n_f - 2 * (k + 1)) % n_f

    for k in range(peers):

        @pl.when(f >= 2 * (k + 1))
        def _():
            pl.semaphore_signal(
                ack.at[k], inc=1, device_id={"fsdp": source_of(f, k)}, device_id_type=MESH
            )

    for j in range(1, n_t):

        @pl.when(t >= j)
        def _():
            pl.semaphore_signal(
                ack_t.at[j], inc=1, device_id={"tm": (t + n_t - j) % n_t}, device_id_type=MESH
            )

    def entered(condition, j):
        @pl.when(condition)
        def _():
            pl.semaphore_wait(ack_t.at[j], 1)

    parity = t % 2
    beside = t + 1 - 2 * parity

    def rows_of(w, source, i, par):
        depth = weights[w][0].shape[0]
        count = pieces_of(depth)
        size = depth // count
        piece = i + par * (count - 1 - 2 * i)
        return pl.ds(pl.multiple_of(source * depth + piece * size, size), size)

    def direct(w, k, i, source):
        src, dst = weights[w]
        return pltpu.make_async_remote_copy(
            src_ref=src.at[rows_of(w, 0, i, parity)],
            dst_ref=dst.at[rows_of(w, source, i, parity)],
            send_sem=w_send.at[w, k, i],
            recv_sem=w_recv.at[w, k, i],
            device_id={"fsdp": (f + 2 * (k + 1)) % n_f},
            device_id_type=MESH,
        )

    def cross(w, k, i, source, par):
        dst = weights[w][1]
        where = rows_of(w, source, i, par)
        return pltpu.make_async_remote_copy(
            src_ref=dst.at[where],
            dst_ref=dst.at[where],
            send_sem=y_send.at[w, k, i],
            recv_sem=y_recv.at[w, k, i],
            device_id={"tm": beside},
            device_id_type=MESH,
        )

    def forward(w, k, i, source, par, slot):
        dst = weights[w][1]
        where = rows_of(w, source, i, par)
        return pltpu.make_async_remote_copy(
            src_ref=dst.at[where],
            dst_ref=dst.at[where],
            send_sem=m_send.at[w, k, slot],
            recv_sem=m_recv.at[w, k, slot],
            device_id={"fsdp": mate},
            device_id_type=MESH,
        )

    def mate_own(w, source):
        src, dst = weights[w]
        depth = src.shape[0]
        return pltpu.make_async_remote_copy(
            src_ref=src,
            dst_ref=dst.at[pl.ds(pl.multiple_of(source * depth, depth), depth)],
            send_sem=o_send.at[w],
            recv_sem=o_recv.at[w],
            device_id={"fsdp": mate},
            device_id_type=MESH,
        )

    def counts(w):
        depth = weights[w][0].shape[0]
        crossed = crossed_of(w, depth)
        return pieces_of(depth) - crossed, crossed

    def send_direct(w):
        for i in range(counts(w)[0]):
            for k in range(peers):
                start(direct(w, k, i, f))

    def relay(w, lo=0, hi=None):
        straight, crossed = counts(w)
        for i in range(lo, straight if hi is None else hi):
            for k in range(peers):
                source = source_of(f, k)
                direct(w, k, i, source).wait_recv()
                if i < crossed:
                    start(cross(w, k, i, source, parity))
                start(forward(w, k, i, source, parity, i))
        if hi is None:
            for i in range(crossed):
                for k in range(peers):
                    source = source_of(f, k)
                    cross(w, k, i, source, 1 - parity).wait_recv()
                    start(forward(w, k, i, source, 1 - parity, straight + i))

    def gathered(w):
        straight, crossed = counts(w)
        own_weights[w].wait()
        mate_own(w, mate).wait_recv()
        for k in range(peers):
            source = source_of(mate, k)
            for i in range(straight):
                forward(w, k, i, source, parity, i).wait_recv()
            for i in range(crossed):
                forward(w, k, i, source, 1 - parity, straight + i).wait_recv()

    def presend():
        return pltpu.make_async_remote_copy(
            src_ref=tok.at[1 - side],
            dst_ref=xv.at[1],
            send_sem=p_send,
            recv_sem=p_recv,
            device_id={"tm": partner},
            device_id_type=MESH,
        )

    def norm(values, gain):
        centre = values - jnp.mean(values, axis=-1, keepdims=True)
        spread = jnp.mean(centre * centre, axis=-1, keepdims=True)
        return (centre * lax.rsqrt(spread + EPSILON) * gain).astype(BF16)

    block = min(rows, 64)

    def norm_spatial(job):
        @pl.loop(0, rows // block)
        def _(i):
            where = pl.ds(pl.multiple_of(i * block, block), block)
            normed[job, where] = norm(xv[job, where].astype(F32), sg[...])

    def attend(read, size, same_place, store):
        lane = lax.broadcasted_iota(jnp.int32, (1, LANES), 1)
        first = lane < HEAD
        dims = (((1,), (1,)), ((), ()))

        @pl.loop(0, inner // LANES, unroll=4)
        def _(i):
            def load(offset):
                return read(pl.ds(pl.multiple_of(offset + i * LANES, LANES), LANES))

            q = load(0) * HEAD ** (-0.5)
            k = load(inner)
            v = load(2 * inner)
            qh = q.astype(BF16).astype(F32)
            ql = pltpu.roll(q - qh, HEAD, 1)
            kh = k.astype(BF16).astype(F32)
            kl = (k - kh).astype(BF16)
            kr = pltpu.roll(kh, HEAD, 1)
            parts = []
            for own in (first, jnp.logical_not(first)):
                high = jnp.where(own, qh, 0.0).astype(BF16)
                left = jnp.concatenate([jnp.where(own, qh, ql).astype(BF16), high], axis=1)
                right = jnp.concatenate([jnp.where(own, kh, kr).astype(BF16), kl], axis=1)
                s = lax.dot_general(left, right, dims, preferred_element_type=F32)
                if same_place is not None:
                    s = jnp.where(same_place, s, -1e30)
                e = jnp.exp(s - jnp.max(s, axis=-1, keepdims=True)).astype(BF16)
                ones = jnp.where(own, v, 1.0).astype(BF16)
                parts.append(jnp.dot(e, ones, preferred_element_type=F32))
            total = pltpu.roll(jnp.where(first, parts[1], parts[0]), HEAD, 1)
            result = jnp.where(first, parts[0], parts[1]) / total
            store(pl.ds(pl.multiple_of(i * LANES, LANES), LANES), result)

    def a2a(kind, s, j, job, to, take, frame):
        return pltpu.make_async_remote_copy(
            src_ref=mid.at[job, take],
            dst_ref=arrived.at[s, frame],
            send_sem=a_send.at[kind, s, j],
            recv_sem=a_recv.at[kind, s, j],
            device_id={"tm": to},
            device_id_type=MESH,
        )

    def own_mid(kind, s, job, take, frame):
        return pltpu.make_async_copy(
            mid.at[job, take], arrived.at[s, frame], own_sem.at[kind, s]
        )

    far_first = sorted(range(1, n_t), key=lambda j: abs(j - half))

    def near(kind, act):
        frame = (t, partner)[kind]
        for s in range(2):
            for j in range(1, half):
                there = (u + j) % half
                act(a2a(kind, s, j, kind, side * half + there, 2 * there + s, frame))
            if act is begin:
                own_mid(kind, s, kind, 2 * u + s, frame).start()

    def wide(s, act):
        job = 2 * s
        for j in far_first:
            to = (t + j) % n_t
            act(a2a(0, s, j, job, to, to, t))
        if act is begin:
            own_mid(0, s, job, t, t).start()

    def begin(cp):
        cp.start()

    def drain(cp):
        cp.wait_send()

    def arrive(s):
        @pl.when(core == 0)
        def _():
            for kind in range(2):
                own_mid(kind, s, kind, 2 * u + s, (t, partner)[kind]).wait()
                for j in range(1, half):
                    source = side * half + (u + half - j) % half
                    frame = (source, (source + half) % n_t)[kind]
                    a2a(kind, s, j, kind, source, 0, frame).wait_recv()

        @pl.when(core == 1)
        def _():
            own_mid(0, s, 2 * s, t, t).wait()
            for j in range(1, n_t):
                source = (t + n_t - j) % n_t
                a2a(0, s, j, 2 * s, source, 0, source).wait_recv()

    def spatial(job):
        @pl.loop(0, 3)
        def _(i):
            cols = pl.ds(pl.multiple_of(i * inner, LANES), inner)
            proj[:, cols] = jnp.dot(normed[job], wsq[:, cols], preferred_element_type=F32)

        def store(cols, result):
            ctx[:, cols] = result.astype(BF16)

        attend(lambda cols: proj[:, cols], rows, None, store)

    def spatial_out(job):
        @pl.loop(0, width // inner)
        def _(i):
            cols = pl.ds(pl.multiple_of(i * inner, LANES), inner)
            part = xv[job, :, cols].astype(F32) + jnp.dot(
                ctx[...], wso[:, cols], preferred_element_type=F32
            )
            mid[job, :, :, cols] = part.reshape(n_t, places, inner).astype(BF16)

    @pl.when(core == 1)
    def _():
        for w in range(4):
            mate_own(w, f).start()

    for k in range(peers):

        @pl.when(f + 2 * (k + 1) < n_f)
        def _():
            pl.semaphore_wait(ack.at[k], 1)

    for w in range(4):
        send_direct(w)
    entered(t < half, half)

    @pl.when(core == 0)
    def _():
        presend().start()

    token_copies[0].wait()
    norm_spatial(0)

    @pl.when(core == 0)
    def _():
        pl.semaphore_wait(ack.at[peers], 1)
        for w in range(4):
            mate_own(w, f).start()

    entered(parity == 0, 1)
    token_copies[1].wait()
    norm_spatial(2)

    relay(0)
    gathered(0)
    for j in range(1, n_t):
        if j != half:
            entered((t + j < n_t) & ((parity == 1) | (j > 1)), j)

    spatial(0)
    relay(1)
    gathered(1)
    spatial_out(0)

    @pl.when(core == 0)
    def _():
        near(0, begin)

    @pl.when(core == 1)
    def _():
        wide(0, begin)


    @pl.when(core == 0)
    def _():
        presend().wait_recv()
        norm_spatial(1)

    spatial(1 + core)
    spatial_out(1 + core)

    @pl.when(core == 0)
    def _():
        near(1, begin)

    @pl.when(core == 1)
    def _():
        wide(1, begin)


    @pl.when(core == 0)
    def _():
        spatial(2)
        spatial_out(2)

    relay(2)

    group = min(places, max(8, LANES // n_t))
    size = n_t * group
    r = lax.rem(lax.broadcasted_iota(jnp.int32, (size, 1), 0), group)
    l = lax.rem(lax.broadcasted_iota(jnp.int32, (1, size), 1), group)
    same_place = r == l

    def back(s, j, to, clip, slot):
        return pltpu.make_async_remote_copy(
            src_ref=ctx_t.at[s, to],
            dst_ref=ctx_back.at[clip, slot],
            send_sem=c_send.at[s, j],
            recv_sem=c_recv.at[s, j],
            device_id={"tm": to},
            device_id_type=MESH,
        )

    def place_of(s):
        return side * (1 - core) + s * core, (2 * u + s) * (1 - core) + t * core

    def own_back(s):
        clip, slot = place_of(s)
        return pltpu.make_async_copy(ctx_t.at[s, t], ctx_back.at[clip, slot], own_sem.at[2, s])

    span = max(1, block // places)
    for s in range(2):
        arrive(s)

        @pl.loop(0, n_t // span)
        def _(i):
            frames = pl.ds(i * span, span)
            values = arrived[s, frames].astype(F32).reshape(span * places, width)
            where = pl.ds(pl.multiple_of(i * span * places, span * places), span * places)
            normed_t[where] = norm(values, tg[...])

        if s == 0:
            gathered(2)

        @pl.loop(0, 3)
        def _(i):
            cols = pl.ds(pl.multiple_of(i * inner, LANES), inner)
            part = jnp.dot(normed_t[...], wtq[:, cols], preferred_element_type=F32)
            proj_t[:, :, cols] = part.reshape(n_t, places, inner)

        for g in range(places // group):
            at = g * group

            def store(cols, result):
                ctx_t[s, :, at : at + group, cols] = result.reshape(n_t, group, LANES).astype(
                    BF16
                )

            attend(
                lambda cols: proj_t[:, at : at + group, cols].reshape(size, LANES),
                size, same_place, store,
            )
        clip, slot = place_of(s)
        for j in far_first:
            back(s, j, (t + j) % n_t, clip, slot).start()
        own_back(s).start()
    relay(3)
    gathered(3)
    for cp in sends:
        cp.wait_send()
    for w in range(4):
        mate_own(w, f).wait_send()

    @pl.when(core == 0)
    def _():
        presend().wait_send()
        near(0, drain)
        near(1, drain)

    @pl.when(core == 1)
    def _():
        wide(0, drain)
        wide(1, drain)

    finals = []
    for e in range(2):
        clip = first_clip if e == 0 else 1 - first_clip

        @pl.when(core == 0)
        def _():
            for s in range(2):
                if e == 0:
                    own_back(s).wait()
                for j in range(1, n_t):
                    source = (t + n_t - j) % n_t

                    @pl.when((source // half == side) == (e == 0))
                    def _():
                        back(s, j, source, source // half, 2 * (source % half) + s).wait_recv()

        @pl.when(core == 1)
        def _():
            own_back(e).wait()
            for j in range(1, n_t):
                source = (t + n_t - j) % n_t
                back(e, j, source, e, source).wait_recv()

        now = ctx_back[clip]
        if places % 16:
            now = now.astype(F32)
        ctx[...] = now.reshape(rows, inner).astype(BF16)

        @pl.loop(0, width // inner)
        def _(i):
            cols = pl.ds(pl.multiple_of(i * inner, LANES), inner)
            base = mid[2 * e, :, :, cols].astype(F32).reshape(rows, inner)
            part = base + jnp.dot(ctx[...], wto[:, cols], preferred_element_type=F32)
            outv[e, :, :, cols] = part.reshape(n_t, places, inner).astype(BF16)

        cp = pltpu.make_async_copy(outv.at[e], out.at[clip], out_sem.at[e])
        cp.start()
        finals.append(cp)
    for s in range(2):
        for j in range(1, n_t):
            back(s, j, (t + j) % n_t, 0, 0).wait_send()
    for cp in finals:
        cp.wait()


def shards(
    n_f, n_t, tokens, spatial_gain, spatial_qkv, spatial_out, temporal_gain, temporal_qkv,
    temporal_out,
):
    clip_count, frames, rows, width = tokens.shape
    assert frames == 1 and clip_count == 2 and n_t % 4 == 0
    inner = spatial_out.shape[0] * n_f
    columns = spatial_qkv.shape[1]
    half = n_t // 2
    places = rows // n_t
    peers = max(1, n_f // 2 - 1)
    most = pieces_of(max(spatial_qkv.shape[0], spatial_out.shape[0]))
    anywhere = pl.BlockSpec(memory_space=pl.ANY)
    vmem = pl.BlockSpec(memory_space=pltpu.VMEM)
    dma = pltpu.SemaphoreType.DMA
    result = pl.pallas_call(
        functools.partial(kernel, n_f, n_t),
        out_shape=jax.ShapeDtypeStruct((clip_count, n_t, places, width), BF16),
        in_specs=[anywhere, vmem, anywhere, anywhere, vmem, anywhere, anywhere],
        out_specs=anywhere,
        scratch_shapes=[
            pltpu.VMEM((3, rows, width), BF16),
            pltpu.VMEM((3, rows, width), BF16),
            pltpu.VMEM((rows, columns), F32),
            pltpu.VMEM((rows, inner), BF16),
            pltpu.VMEM((3, n_t, places, width), BF16),
            pltpu.VMEM((2, n_t, places, width), BF16),
            pltpu.VMEM((rows, width), BF16),
            pltpu.VMEM((n_t, places, columns), F32),
            pltpu.VMEM((2, n_t, places, inner), BF16),
            pltpu.VMEM((2, n_t, places, inner), BF16),
            pltpu.VMEM((width, columns), BF16),
            pltpu.VMEM((inner, width), BF16),
            pltpu.VMEM((width, columns), BF16),
            pltpu.VMEM((inner, width), BF16),
            pltpu.VMEM((2, n_t, places, width), BF16),
            pltpu.SemaphoreType.REGULAR((peers + 1,)),
            pltpu.SemaphoreType.REGULAR((n_t,)),
            dma((3,)),
            dma((4,)),
            dma((4, peers, most)),
            dma((4, peers, most)),
            dma((4, peers, most)),
            dma((4, peers, most)),
            dma((4, peers, most)),
            dma((4, peers, most)),
            dma((4,)),
            dma((4,)),
            dma,
            dma,
            dma((2, 2, n_t)),
            dma((2, 2, n_t)),
            dma((2, n_t)),
            dma((2, n_t)),
            dma((3, 2)),
            dma((2,)),
        ],
        compiler_params=pltpu.CompilerParams(
            collective_id=0, has_side_effects=True, vmem_limit_bytes=67000000
        ),
    )(
        tokens.reshape(clip_count, rows, width),
        spatial_gain.reshape(1, width),
        spatial_qkv,
        spatial_out,
        temporal_gain.reshape(1, width),
        temporal_qkv,
        temporal_out,
    )
    return result.reshape(clip_count, frames, rows, width)


def solution(mesh):
    placed = (
        P("fsdp", "tm", None, None),
        P(),
        P("fsdp", None),
        P("fsdp", None),
        P(),
        P("fsdp", None),
        P("fsdp", None),
    )
    body = functools.partial(shards, mesh.shape["fsdp"], mesh.shape["tm"])
    return jax.shard_map(
        body, mesh=mesh, in_specs=placed, out_specs=P("fsdp", "tm", None, None), check_vma=False
    )
```
